32 devices in a mesh: rep: 4 (over z), row: 4 (over x, core), col: 2 (over y).
Axes of the slice: x: 2, y: 2, z: 4, core: 2. Of those that a mesh axis runs over, the one named last changes fastest.
Arguments:
- grad_parts: bfloat16 [4, 16384, 6144], P('rep', ('row', 'col')), may hold values from -0.03125 to 0.03125, as said below
- statistic: float32 [6144, 6144], P('row', 'col'), may hold values from -150 to 150, as said below
Outputs:
- gram_matrix: float32 [6144, 6144], P('row', 'col')
- statistic_next: float32 [6144, 6144], P('row', 'col')
The draws below stay inside these ranges and needn't reach their ends.
Inputs may be any that keep to these rules, and one draw needn't show every extreme that they name: Every entry of grad_parts has a magnitude between 2^-10 and 2^-5. statistic is symmetric and positive definite.
All inputs are finite; a program needn't handle non-finite values.
Results may differ from the reference program's by a relative error of at most 0.008.
Values may be sent and summed in bfloat16 or wider, within the bound.
A program may use at most 192 MiB of HBM per device.

```python
import math
import jax
import jax.numpy as jnp
from jax import lax

D = 6144
HID = 16384
N_REP = 4


def draw_grad_parts(key, part):
    key_sign = jax.random.fold_in(key, 41)
    key_level = jax.random.fold_in(key, 53)
    signs = jnp.where(jax.random.bernoulli(key_sign, 0.5, (N_REP, HID, D)), 1.0, -1.0).astype(jnp.float32)
    level = jax.random.uniform(key_level, (N_REP, HID, D), jnp.float32, -10.0, -5.0)
    return (signs * jnp.exp2(level)).astype(jnp.bfloat16)


def draw_statistic(key, part):
    key_factor = jax.random.fold_in(key, 11)
    key_ridge = jax.random.fold_in(key, 23)
    factor = jax.random.truncated_normal(key_factor, -3.0, 3.0, (D, D), jnp.float32) * (2.0 / math.sqrt(D))
    crossed = jnp.dot(factor.T, factor, precision=lax.Precision.HIGHEST)
    crossed = 0.5 * (crossed + crossed.T)
    ridge = jax.random.uniform(key_ridge, (D,), jnp.float32, 0.25, 1.0)
    return crossed + jnp.diag(ridge)


def setup_inputs(seed: int = 0) -> dict:
    seeds = jax.random.split(jax.random.key(seed), 3)
    grad_parts = draw_grad_parts(jax.random.fold_in(seeds[2], 71), 0)
    statistic = draw_statistic(jax.random.fold_in(seeds[2], 71), 0)
    return {"grad_parts": grad_parts, "statistic": statistic}


def reference(grad_parts, statistic):
    summed = jnp.sum(grad_parts.astype(jnp.float32), axis=0).astype(jnp.bfloat16)
    summed = lax.optimization_barrier(summed)
    summed_f32 = summed.astype(jnp.float32)
    product = jnp.dot(summed_f32.T, summed_f32, precision=lax.Precision.HIGHEST)
    gram_full = 0.5 * (product + product.T)
    statistic_next = 0.95 * statistic + 0.05 * gram_full
    return gram_full, statistic_next
```

```python
import functools

import jax
import jax.numpy as jnp
from jax import lax
from jax.experimental import pallas as pl
from jax.experimental.pallas import tpu as pltpu
from jax.sharding import PartitionSpec as P

ITEMS = 32
MIDDLE = 4
BANDS = 6
PARTS = 2
SLABS = 4
CHUNK = 1536
STRIP = 16
VMEM_LIMIT = 62 * 2**20
MESH = pl.DeviceIdType.MESH


def plan(reps):
    middle = MIDDLE if reps > 2 else 0
    end = (ITEMS - (reps - 2) * middle) // 2
    return end, middle, end + (reps - 2) * middle


def bits_of(axis, size):
    bits, bit = [], size // 2
    while bit:
        bits.append((axis, bit))
        bit //= 2
    return bits


def digit(axis, bit):
    return lax.rem(lax.axis_index(axis) // bit, 2)


def partner(axis, bit):
    return {axis: lax.axis_index(axis) + bit - 2 * bit * digit(axis, bit)}


def greet(bits, reps, others=()):
    here = lax.axis_index("rep")
    barrier = pltpu.get_barrier_semaphore()

    def signal(device):
        pl.semaphore_signal(barrier, inc=1, device_id=device, device_id_type=MESH)

    for axis, bit in bits:
        signal(partner(axis, bit))
    for device in others:
        signal(device)
    pl.when(here > 0)(lambda: signal({"rep": here - 1}))
    pl.when(here < reps - 1)(lambda: signal({"rep": here + 1}))
    ends = jnp.where(here > 0, 1, 0) + jnp.where(here < reps - 1, 1, 0)
    pl.semaphore_wait(barrier, len(bits) + len(others) + ends)


def add_strips(out, *refs):
    rows = out.shape[0]

    def strip(n, carry):
        at = pl.ds(pl.multiple_of(n * STRIP, STRIP), STRIP)
        total = refs[0][at, :].astype(jnp.float32)
        for ref in refs[1:]:
            total = total + ref[at, :].astype(jnp.float32)
        out[at, :] = total.astype(out.dtype)
        return carry

    lax.fori_loop(0, rows // STRIP, strip, 0)


def collect_kernel(
    reps, bits, orders, own, out, ups, downs, loads, zeros,
    load_sem, up_send, up_recv, down_send, down_recv, hop_send, hop_recv, keep_sem, zero_sem,
):
    end, middle, length = plan(reps)
    here = lax.axis_index("rep")
    mirror = reps - 1 - here
    at_end = (here == 0) | (here == reps - 1)
    inside = (here > 0) & (here < reps - 1)
    size, width = loads.shape[1], loads.shape[2]
    half = width // 2
    kept = jnp.where(at_end, end, middle)
    base = jnp.where(at_end, reps - 1, end + middle + 1)

    greet(bits, reps)

    def rows(position):
        return own.at[pl.ds(pl.multiple_of(position * size, size), size), :]

    def load(slot, position):
        return pltpu.make_async_copy(rows(position), loads.at[slot], load_sem.at[slot])

    def chain(slots, send, recv, j, to, source=None):
        return pltpu.make_async_remote_copy(
            src_ref=slots.at[j] if source is None else source,
            dst_ref=slots.at[j],
            send_sem=send.at[j],
            recv_sem=recv.at[j],
            device_id={"rep": to},
            device_id_type=MESH,
        )

    def go_up(j, source=None):
        return chain(ups, up_send, up_recv, j, here + 1, source)

    def go_down(j, source=None):
        return chain(downs, down_send, down_recv, j, here - 1, source)

    def up_items(place):
        return jnp.where(place < reps - 1, end + (reps - 2 - place) * middle, 0)

    def place_of(f, exchanged, h):
        index = [f]
        for axis, bit in bits:
            index.append(slice(None) if (axis, bit) in exchanged else digit(axis, bit))
        index.append(slice(None))
        index.append(pl.ds(h * half, half))
        return out.at[tuple(index)]

    def hop(f, h, stage, source=None):
        order = orders[h]
        spot = place_of(f, order[:stage], h)
        return pltpu.make_async_remote_copy(
            src_ref=spot if source is None else source,
            dst_ref=spot,
            send_sem=hop_send.at[f, h, stage],
            recv_sem=hop_recv.at[f, h, stage],
            device_id=partner(*order[stage]),
            device_id_type=MESH,
        )

    def keep(f, source):
        index = tuple([f] + [digit(axis, bit) for axis, bit in bits])
        return pltpu.make_async_copy(source, out.at[index], keep_sem.at[f])

    def spread(f, source):
        for h in range(2):
            hop(f, h, 0, source.at[:, pl.ds(h * half, half)]).start()
        keep(f, source).start()

    spare = end - middle
    if spare:

        @pl.when(inside)
        def _():
            zeros[...] = jnp.zeros_like(zeros)

            def fill(n, carry):
                left, index = n, []
                for _ in bits:
                    index.append(lax.rem(left, 2))
                    left = left // 2
                at = tuple([middle + left] + index)
                pltpu.make_async_copy(zeros, out.at[at], zero_sem).start()
                return carry

            lax.fori_loop(0, spare * 2 ** len(bits), fill, 0)

    stages = len(bits)
    ticks = max(
        length + reps - 2,
        reps + stages + (3 * (end - 1)) // 2,
        (end + middle + 2 + stages + (3 * (middle - 1)) // 2) if middle else 0,
    )

    def tick(t, carry):
        up_j, down_j = t - here, t - mirror
        up_on = (up_j >= 0) & (up_j < up_items(here))
        down_on = (down_j >= 0) & (down_j < up_items(mirror))
        f = t - base
        final_on = (f >= 0) & (f < kept)
        late = here * 2 >= reps
        offset = jnp.where(late, f, middle - 1 - f)
        position = jnp.where(
            here == 0, f, jnp.where(mirror == 0, ITEMS - 1 - f, end + (here - 1) * middle + offset)
        )

        pl.when(up_on & (here > 0))(lambda: load(0, ITEMS - 1 - up_j).start())
        pl.when(down_on & (mirror > 0))(lambda: load(1, down_j).start())
        pl.when(final_on)(lambda: load(2, position).start())

        pl.when(up_on & (here == 0))(lambda: go_up(up_j, rows(ITEMS - 1 - up_j)).start())
        pl.when(down_on & (mirror == 0))(lambda: go_down(down_j, rows(down_j)).start())

        @pl.when(up_on & (here > 0))
        def _():
            load(0, ITEMS - 1 - up_j).wait()
            go_up(up_j).wait_recv()
            slot = ups.at[up_j]
            add_strips(slot, slot, loads.at[0])
            go_up(up_j).start()

        @pl.when(down_on & (mirror > 0))
        def _():
            load(1, down_j).wait()
            go_down(down_j).wait_recv()
            slot = downs.at[down_j]
            add_strips(slot, slot, loads.at[1])
            go_down(down_j).start()

        @pl.when(final_on & (here == 0))
        def _():
            load(2, position).wait()
            go_down(f).wait_recv()
            add_strips(downs.at[f], downs.at[f], loads.at[2])
            spread(f, downs.at[f])

        @pl.when(final_on & (mirror == 0))
        def _():
            load(2, position).wait()
            go_up(f).wait_recv()
            add_strips(ups.at[f], ups.at[f], loads.at[2])
            spread(f, ups.at[f])

        @pl.when(final_on & inside)
        def _():
            load(2, position).wait()
            up, down = ITEMS - 1 - position, position
            go_up(up).wait_recv()
            go_down(down).wait_recv()
            add_strips(ups.at[up], ups.at[up], downs.at[down], loads.at[2])
            spread(f, ups.at[up])

        for stage in range(1, stages + 1):
            m = t - base - stage
            g = 2 * (m // 3) + lax.rem(m, 3)

            @pl.when((m >= 0) & (lax.rem(m, 3) < 2) & (g < kept))
            def _():
                for h in range(2):
                    hop(g, h, stage - 1).wait_recv()
                    hop(g, h, stage - 1).wait_send()
                if stage == 1:
                    keep(g, loads.at[2]).wait()
                if stage < stages:
                    for h in range(2):
                        hop(g, h, stage).start()

        return carry

    lax.fori_loop(0, ticks, tick, 0)

    def drain(j, carry):
        pl.when(j < up_items(here))(lambda: go_up(j).wait_send())
        pl.when(j < up_items(mirror))(lambda: go_down(j).wait_send())
        return carry

    lax.fori_loop(0, length, drain, 0)
    if spare:

        @pl.when(inside)
        def _():
            spot = out.at[pl.ds(middle, spare)]
            pltpu.make_async_copy(spot, spot, zero_sem).wait()


def collect(own):
    reps = lax.axis_size("rep")
    end, middle, length = plan(reps)
    row_bits = bits_of("row", lax.axis_size("row"))
    col_bits = bits_of("col", lax.axis_size("col"))
    bits = row_bits + col_bits
    orders = (col_bits + row_bits, row_bits[:-1] + col_bits + row_bits[-1:])
    size, width = own.shape[0] // ITEMS, own.shape[1]
    dma = pltpu.SemaphoreType.DMA
    gathered = pl.pallas_call(
        functools.partial(collect_kernel, reps, bits, orders),
        out_shape=jax.ShapeDtypeStruct((end,) + (2,) * len(bits) + (size, width), own.dtype),
        in_specs=[pl.BlockSpec(memory_space=pl.ANY)],
        out_specs=pl.BlockSpec(memory_space=pl.ANY),
        scratch_shapes=[
            pltpu.VMEM((length, size, width), own.dtype),
            pltpu.VMEM((length, size, width), own.dtype),
            pltpu.VMEM((3, size, width), own.dtype),
            pltpu.VMEM((size, width), own.dtype),
            dma((3,)),
            dma((length,)),
            dma((length,)),
            dma((length,)),
            dma((length,)),
            dma((end, 2, len(bits))),
            dma((end, 2, len(bits))),
            dma((end,)),
            dma,
        ],
        compiler_params=pltpu.CompilerParams(
            collective_id=0, has_side_effects=True, vmem_limit_bytes=VMEM_LIMIT
        ),
    )(own)
    return gathered.reshape(-1, width)


def total_kernel(
    reps, rows, cols, shared, summed, out, held, ups, downs, sends, left, right, turned,
    left_sem, right_sem, out_sem, up_send, up_recv, down_send, down_recv, *extra,
):
    here = lax.axis_index("rep")
    mirror = reps - 1 - here
    bands, size, band_cols = held.shape
    depth = left.shape[1]
    slabs = summed.shape[0] // depth
    chunk = min(CHUNK, band_cols)
    row, col = lax.axis_index("row"), lax.axis_index("col")
    if shared:
        given, taken, square, pair_send, pair_recv, square_sem = extra
        twin_row = jnp.where(row // 2 == col, row + 1 - 2 * lax.rem(row, 2), 2 * col + lax.rem(row, 2))
        twin = {"row": twin_row, "col": row // 2}
        low = row < twin_row
        twin_place = (twin_row - 2 * col) * rows
        own_place = rows - twin_place
        half = rows // 2
    else:
        own_place = 0

    def starts(k):
        plain = row * rows + (k - shared) * size, col * cols + own_place
        if not shared:
            return plain
        first = jnp.where(low, row * rows, twin_row * rows + half) + k * size
        second = jnp.where(low, twin_row, row) * rows
        is_shared = k < shared
        return jnp.where(is_shared, first, plain[0]), jnp.where(is_shared, second, plain[1])

    def fetch(k, n, slot):
        along = pl.ds(pl.multiple_of(n * depth, depth), depth)
        down, across = starts(k)
        return (
            pltpu.make_async_copy(
                summed.at[along, pl.ds(pl.multiple_of(down, 128), size)],
                left.at[slot],
                left_sem.at[slot],
            ),
            pltpu.make_async_copy(
                summed.at[along, pl.ds(pl.multiple_of(across, 128), band_cols)],
                right.at[slot],
                right_sem.at[slot],
            ),
        )

    def start(copies):
        for copy in copies:
            copy.start()

    def multiply(k):
        def slab(n, carry):
            slot = lax.rem(n, 2)
            pl.when(n + 1 < slabs)(lambda: start(fetch(k, n + 1, 1 - slot)))
            pl.when((n + 1 == slabs) & (k + 1 < bands))(lambda: start(fetch(k + 1, 0, 1 - slot)))
            for copy in fetch(k, n, slot):
                copy.wait()
            turned[...] = left[slot].T * 2
            for c in range(0, band_cols, chunk):
                at = pl.ds(c, chunk)
                held[k, :, at] += jnp.dot(
                    turned[...], right[slot, :, at], preferred_element_type=jnp.float32
                )
            return carry

        held[k] = jnp.zeros(held.shape[1:], held.dtype)
        lax.fori_loop(0, slabs, slab, 0)

    def store(k):
        at = pl.ds(pl.multiple_of((k - shared) * size, size), size)
        across = pl.ds(pl.multiple_of(own_place, 128), band_cols)
        return pltpu.make_async_copy(held.at[k], out.at[at, across], out_sem.at[k])

    part_cols = band_cols // PARTS

    def part(ref, p):
        return ref.at[:, pl.ds(p * part_cols, part_cols)]

    def hop(side, k, p):
        return pltpu.make_async_remote_copy(
            src_ref=part(sends.at[side, lax.rem(k, 2)], p),
            dst_ref=part((ups, downs)[side].at[k], p),
            send_sem=(up_send, down_send)[side].at[k, p],
            recv_sem=(up_recv, down_recv)[side].at[k, p],
            device_id={"rep": (here + 1, here - 1)[side]},
            device_id_type=MESH,
        )

    def swap(k):
        return pltpu.make_async_remote_copy(
            src_ref=given.at[k],
            dst_ref=taken.at[k],
            send_sem=pair_send.at[k],
            recv_sem=pair_recv.at[k],
            device_id=twin,
            device_id_type=MESH,
        )

    def put(source, k, first):
        at = pl.ds(pl.multiple_of(jnp.where(first, 0, half) + k * size, size), size)

        @pl.when(low)
        def _():
            add_strips(square.at[at, :], source)

        @pl.when(jnp.logical_not(low))
        def _():
            def turn(n, carry):
                along = pl.ds(pl.multiple_of(n * 128, 128), 128)
                square[along, at] = source[:, along].astype(jnp.float32).T
                return carry

            lax.fori_loop(0, rows // 128, turn, 0)

    greet([], reps, [twin] if shared else [])
    start(fetch(0, 0, 0))
    multiply(0)

    def tick(t, carry):
        for p in range(PARTS):
            for side, depth in ((0, here), (1, mirror)):
                k = t - depth
                on = (k >= 0) & (k < bands) & (depth < reps - 1)
                pl.when(on & (k >= 2))(lambda: hop(side, k - 2, p).wait_send())
                buffer = part(sends.at[side, lax.rem(k + bands * reps * 2, 2)], p)

                @pl.when(on & (depth == 0))
                def _():
                    add_strips(buffer, part(held.at[k], p))
                    hop(side, k, p).start()

                @pl.when(on & (depth > 0))
                def _():
                    hop(side, k, p).wait_recv()
                    add_strips(buffer, part(held.at[k], p), part((ups, downs)[side].at[k], p))
                    hop(side, k, p).start()

        k = t - jnp.maximum(here, mirror)
        on = (k >= 0) & (k < bands)

        @pl.when(on & (here == 0))
        def _():
            for p in range(PARTS):
                hop(1, k, p).wait_recv()
            add_strips(held.at[k], held.at[k], downs.at[k])

        @pl.when(on & (mirror == 0))
        def _():
            for p in range(PARTS):
                hop(0, k, p).wait_recv()
            add_strips(held.at[k], held.at[k], ups.at[k])

        @pl.when(on & (here > 0) & (mirror > 0))
        def _():
            add_strips(held.at[k], held.at[k], ups.at[k], downs.at[k])

        pl.when(on & (k >= shared))(lambda: store(k).start())
        if shared:

            @pl.when(on & (k < shared))
            def _():
                add_strips(given.at[k], held.at[k])
                swap(k).start()
                put(held.at[k], k, low)

        pl.when(t + 1 < bands)(lambda: multiply(t + 1))
        return carry

    lax.fori_loop(0, bands + reps - 1, tick, 0)
    if shared:
        for k in range(shared):
            swap(k).wait()
            put(taken.at[k], k, jnp.logical_not(low))
        across = pl.ds(pl.multiple_of(twin_place, 128), rows)
        copy = pltpu.make_async_copy(square, out.at[:, across], square_sem)
        copy.start()
    for side, depth in ((0, here), (1, mirror)):
        for k in range(max(bands - 2, 0), bands):
            for p in range(PARTS):
                pl.when(depth < reps - 1)(lambda: hop(side, k, p).wait_send())

    def finish(k, carry):
        store(k).wait()
        return carry

    lax.fori_loop(shared, bands, finish, 0)
    if shared:
        copy.wait()


def total(summed, rows, cols):
    reps = lax.axis_size("rep")
    paired = cols == 2 * rows and lax.axis_size("row") == 2 * lax.axis_size("col")
    shared = BANDS // 2 if paired else 0
    bands, size = BANDS + shared, rows // BANDS
    band_cols = rows if paired else cols
    depth = summed.shape[0] // SLABS
    dma = pltpu.SemaphoreType.DMA
    shape = (bands, size, band_cols)
    extra = [
        pltpu.VMEM((shared, size, band_cols), jnp.bfloat16),
        pltpu.VMEM((shared, size, band_cols), jnp.bfloat16),
        pltpu.VMEM((rows, rows), jnp.float32),
        dma((max(shared, 1),)),
        dma((max(shared, 1),)),
        dma,
    ]
    return pl.pallas_call(
        functools.partial(total_kernel, reps, rows, cols, shared),
        out_shape=jax.ShapeDtypeStruct((rows, cols), jnp.float32),
        in_specs=[pl.BlockSpec(memory_space=pl.ANY)],
        out_specs=pl.BlockSpec(memory_space=pl.ANY),
        scratch_shapes=[
            pltpu.VMEM(shape, jnp.float32),
            pltpu.VMEM(shape, jnp.bfloat16),
            pltpu.VMEM(shape, jnp.bfloat16),
            pltpu.VMEM((2, 2) + shape[1:], jnp.bfloat16),
            pltpu.VMEM((2, depth, size), summed.dtype),
            pltpu.VMEM((2, depth, band_cols), summed.dtype),
            pltpu.VMEM((size, depth), summed.dtype),
            dma((2,)),
            dma((2,)),
        ]
        + [dma((bands,))]
        + [dma((bands, PARTS))] * 4
        + (extra if paired else []),
        compiler_params=pltpu.CompilerParams(
            collective_id=1, has_side_effects=True, vmem_limit_bytes=VMEM_LIMIT
        ),
    )(summed)


def shards(grad_parts, statistic):
    tile_rows, tile_cols = statistic.shape
    summed = collect(grad_parts[0])
    gram = 0.5 * total(summed, tile_rows, tile_cols)
    return (gram, 0.95 * statistic + 0.05 * gram)


def solution(mesh):
    return jax.shard_map(
        shards,
        mesh=mesh,
        in_specs=(P("rep", ("row", "col"), None), P("row", "col")),
        out_specs=(P("row", "col"), P("row", "col")),
        check_vma=False,
    )
```

```python
import functools

import jax
import jax.numpy as jnp
from jax import lax
from jax.experimental import pallas as pl
from jax.experimental.pallas import tpu as pltpu
from jax.sharding import PartitionSpec as P

ITEMS = 32
MIDDLE = 4
BANDS = 6
PARTS = 2
LAG = 3
SLABS = 4
CHUNK = 1536
STRIP = 16
VMEM_LIMIT = 62 * 2**20
MESH = pl.DeviceIdType.MESH


def plan(reps):
    middle = MIDDLE if reps > 2 else 0
    end = (ITEMS - (reps - 2) * middle) // 2
    return end, middle, end + (reps - 2) * middle


def bits_of(axis, size):
    bits, bit = [], size // 2
    while bit:
        bits.append((axis, bit))
        bit //= 2
    return bits


def digit(axis, bit):
    return lax.rem(lax.axis_index(axis) // bit, 2)


def partner(axis, bit):
    return {axis: lax.axis_index(axis) + bit - 2 * bit * digit(axis, bit)}


def greet(bits, reps, others=()):
    here = lax.axis_index("rep")
    barrier = pltpu.get_barrier_semaphore()

    def signal(device):
        pl.semaphore_signal(barrier, inc=1, device_id=device, device_id_type=MESH)

    for axis, bit in bits:
        signal(partner(axis, bit))
    for device in others:
        signal(device)
    pl.when(here > 0)(lambda: signal({"rep": here - 1}))
    pl.when(here < reps - 1)(lambda: signal({"rep": here + 1}))
    ends = jnp.where(here > 0, 1, 0) + jnp.where(here < reps - 1, 1, 0)
    pl.semaphore_wait(barrier, len(bits) + len(others) + ends)


def add_strips(out, *refs):
    rows = out.shape[0]

    def strip(n, carry):
        at = pl.ds(pl.multiple_of(n * STRIP, STRIP), STRIP)
        total = refs[0][at, :].astype(jnp.float32)
        for ref in refs[1:]:
            total = total + ref[at, :].astype(jnp.float32)
        out[at, :] = total.astype(out.dtype)
        return carry

    lax.fori_loop(0, rows // STRIP, strip, 0)


def collect_kernel(
    reps, bits, orders, own, out, ups, downs, loads, zeros,
    load_sem, up_send, up_recv, down_send, down_recv, hop_send, hop_recv, keep_sem, zero_sem,
):
    end, middle, length = plan(reps)
    here = lax.axis_index("rep")
    mirror = reps - 1 - here
    at_end = (here == 0) | (here == reps - 1)
    inside = (here > 0) & (here < reps - 1)
    size, width = loads.shape[1], loads.shape[2]
    half = width // 2
    kept = jnp.where(at_end, end, middle)
    base = jnp.where(at_end, reps - 1, end + middle + 1)

    greet(bits, reps)

    def rows(position):
        return own.at[pl.ds(pl.multiple_of(position * size, size), size), :]

    def load(slot, position):
        return pltpu.make_async_copy(rows(position), loads.at[slot], load_sem.at[slot])

    def chain(slots, send, recv, j, to, source=None):
        return pltpu.make_async_remote_copy(
            src_ref=slots.at[j] if source is None else source,
            dst_ref=slots.at[j],
            send_sem=send.at[j],
            recv_sem=recv.at[j],
            device_id={"rep": to},
            device_id_type=MESH,
        )

    def go_up(j, source=None):
        return chain(ups, up_send, up_recv, j, here + 1, source)

    def go_down(j, source=None):
        return chain(downs, down_send, down_recv, j, here - 1, source)

    def up_items(place):
        return jnp.where(place < reps - 1, end + (reps - 2 - place) * middle, 0)

    def place_of(f, exchanged, h):
        index = [f]
        for axis, bit in bits:
            index.append(slice(None) if (axis, bit) in exchanged else digit(axis, bit))
        index.append(slice(None))
        index.append(pl.ds(h * half, half))
        return out.at[tuple(index)]

    def hop(f, h, stage, source=None):
        order = orders[h]
        spot = place_of(f, order[:stage], h)
        return pltpu.make_async_remote_copy(
            src_ref=spot if source is None else source,
            dst_ref=spot,
            send_sem=hop_send.at[f, h, stage],
            recv_sem=hop_recv.at[f, h, stage],
            device_id=partner(*order[stage]),
            device_id_type=MESH,
        )

    def keep(f, source):
        index = tuple([f] + [digit(axis, bit) for axis, bit in bits])
        return pltpu.make_async_copy(source, out.at[index], keep_sem.at[f])

    def spread(f, source):
        for h in range(2):
            hop(f, h, 0, source.at[:, pl.ds(h * half, half)]).start()
        keep(f, source).start()

    spare = end - middle
    if spare:

        @pl.when(inside)
        def _():
            zeros[...] = jnp.zeros_like(zeros)

            def fill(n, carry):
                left, index = n, []
                for _ in bits:
                    index.append(lax.rem(left, 2))
                    left = left // 2
                at = tuple([middle + left] + index)
                pltpu.make_async_copy(zeros, out.at[at], zero_sem).start()
                return carry

            lax.fori_loop(0, spare * 2 ** len(bits), fill, 0)

    stages = len(bits)
    ticks = max(
        length + reps - 2,
        reps + stages + (3 * (end - 1)) // 2,
        (end + middle + 2 + stages + (3 * (middle - 1)) // 2) if middle else 0,
    )

    def tick(t, carry):
        up_j, down_j = t - here, t - mirror
        up_on = (up_j >= 0) & (up_j < up_items(here))
        down_on = (down_j >= 0) & (down_j < up_items(mirror))
        f = t - base
        final_on = (f >= 0) & (f < kept)
        late = here * 2 >= reps
        offset = jnp.where(late, f, middle - 1 - f)
        position = jnp.where(
            here == 0, f, jnp.where(mirror == 0, ITEMS - 1 - f, end + (here - 1) * middle + offset)
        )

        pl.when(up_on & (here > 0))(lambda: load(0, ITEMS - 1 - up_j).start())
        pl.when(down_on & (mirror > 0))(lambda: load(1, down_j).start())
        pl.when(final_on)(lambda: load(2, position).start())

        pl.when(up_on & (here == 0))(lambda: go_up(up_j, rows(ITEMS - 1 - up_j)).start())
        pl.when(down_on & (mirror == 0))(lambda: go_down(down_j, rows(down_j)).start())

        @pl.when(up_on & (here > 0))
        def _():
            load(0, ITEMS - 1 - up_j).wait()
            go_up(up_j).wait_recv()
            slot = ups.at[up_j]
            add_strips(slot, slot, loads.at[0])
            go_up(up_j).start()

        @pl.when(down_on & (mirror > 0))
        def _():
            load(1, down_j).wait()
            go_down(down_j).wait_recv()
            slot = downs.at[down_j]
            add_strips(slot, slot, loads.at[1])
            go_down(down_j).start()

        @pl.when(final_on & (here == 0))
        def _():
            load(2, position).wait()
            go_down(f).wait_recv()
            add_strips(downs.at[f], downs.at[f], loads.at[2])
            spread(f, downs.at[f])

        @pl.when(final_on & (mirror == 0))
        def _():
            load(2, position).wait()
            go_up(f).wait_recv()
            add_strips(ups.at[f], ups.at[f], loads.at[2])
            spread(f, ups.at[f])

        @pl.when(final_on & inside)
        def _():
            load(2, position).wait()
            up, down = ITEMS - 1 - position, position
            go_up(up).wait_recv()
            go_down(down).wait_recv()
            add_strips(ups.at[up], ups.at[up], downs.at[down], loads.at[2])
            spread(f, ups.at[up])

        for stage in range(1, stages + 1):
            m = t - base - stage
            g = 2 * (m // 3) + lax.rem(m, 3)

            @pl.when((m >= 0) & (lax.rem(m, 3) < 2) & (g < kept))
            def _():
                for h in range(2):
                    hop(g, h, stage - 1).wait_recv()
                    hop(g, h, stage - 1).wait_send()
                if stage == 1:
                    keep(g, loads.at[2]).wait()
                if stage < stages:
                    for h in range(2):
                        hop(g, h, stage).start()

        return carry

    lax.fori_loop(0, ticks, tick, 0)

    def drain(j, carry):
        pl.when(j < up_items(here))(lambda: go_up(j).wait_send())
        pl.when(j < up_items(mirror))(lambda: go_down(j).wait_send())
        return carry

    lax.fori_loop(0, length, drain, 0)
    if spare:

        @pl.when(inside)
        def _():
            spot = out.at[pl.ds(middle, spare)]
            pltpu.make_async_copy(spot, spot, zero_sem).wait()


def collect(own):
    reps = lax.axis_size("rep")
    end, middle, length = plan(reps)
    row_bits = bits_of("row", lax.axis_size("row"))
    col_bits = bits_of("col", lax.axis_size("col"))
    bits = row_bits + col_bits
    orders = (col_bits + row_bits, row_bits[:-1] + col_bits + row_bits[-1:])
    size, width = own.shape[0] // ITEMS, own.shape[1]
    dma = pltpu.SemaphoreType.DMA
    gathered = pl.pallas_call(
        functools.partial(collect_kernel, reps, bits, orders),
        out_shape=jax.ShapeDtypeStruct((end,) + (2,) * len(bits) + (size, width), own.dtype),
        in_specs=[pl.BlockSpec(memory_space=pl.ANY)],
        out_specs=pl.BlockSpec(memory_space=pl.ANY),
        scratch_shapes=[
            pltpu.VMEM((length, size, width), own.dtype),
            pltpu.VMEM((length, size, width), own.dtype),
            pltpu.VMEM((3, size, width), own.dtype),
            pltpu.VMEM((size, width), own.dtype),
            dma((3,)),
            dma((length,)),
            dma((length,)),
            dma((length,)),
            dma((length,)),
            dma((end, 2, len(bits))),
            dma((end, 2, len(bits))),
            dma((end,)),
            dma,
        ],
        compiler_params=pltpu.CompilerParams(
            collective_id=0, has_side_effects=True, vmem_limit_bytes=VMEM_LIMIT
        ),
    )(own)
    return gathered.reshape(-1, width)


def total_kernel(
    reps, rows, cols, shared, summed, out, held, ups, downs, sends, left, right, turned,
    left_sem, right_sem, out_sem, up_send, up_recv, down_send, down_recv, *extra,
):
    here = lax.axis_index("rep")
    mirror = reps - 1 - here
    bands, size, band_cols = held.shape
    depth = left.shape[1]
    end, middle, _ = plan(reps)
    valid = middle * (summed.shape[0] // end)
    slabs = summed.shape[0] // depth
    fewer = min(slabs, 2 * pl.cdiv(valid, 2 * depth))
    slabs = jnp.where((here > 0) & (mirror > 0), fewer, slabs)
    chunk = min(CHUNK, band_cols)
    row, col = lax.axis_index("row"), lax.axis_index("col")
    if shared:
        given, taken, square, pair_send, pair_recv, square_sem = extra
        twin_row = jnp.where(row // 2 == col, row + 1 - 2 * lax.rem(row, 2), 2 * col + lax.rem(row, 2))
        twin = {"row": twin_row, "col": row // 2}
        low = row < twin_row
        twin_place = (twin_row - 2 * col) * rows
        own_place = rows - twin_place
        half = rows // 2
    else:
        own_place = 0

    def starts(k):
        plain = row * rows + (k - shared) * size, col * cols + own_place
        if not shared:
            return plain
        first = jnp.where(low, row * rows, twin_row * rows + half) + k * size
        second = jnp.where(low, twin_row, row) * rows
        is_shared = k < shared
        return jnp.where(is_shared, first, plain[0]), jnp.where(is_shared, second, plain[1])

    def fetch(k, n, slot):
        along = pl.ds(pl.multiple_of(n * depth, depth), depth)
        down, across = starts(k)
        return (
            pltpu.make_async_copy(
                summed.at[along, pl.ds(pl.multiple_of(down, 128), size)],
                left.at[slot],
                left_sem.at[slot],
            ),
            pltpu.make_async_copy(
                summed.at[along, pl.ds(pl.multiple_of(across, 128), band_cols)],
                right.at[slot],
                right_sem.at[slot],
            ),
        )

    def start(copies):
        for copy in copies:
            copy.start()

    def multiply(k):
        def slab(n, carry):
            slot = lax.rem(n, 2)
            pl.when(n + 1 < slabs)(lambda: start(fetch(k, n + 1, 1 - slot)))
            pl.when((n + 1 == slabs) & (k + 1 < bands))(lambda: start(fetch(k + 1, 0, 1 - slot)))
            for copy in fetch(k, n, slot):
                copy.wait()
            turned[...] = left[slot].T * 2
            for c in range(0, band_cols, chunk):
                at = pl.ds(c, chunk)
                held[k, :, at] += jnp.dot(
                    turned[...], right[slot, :, at], preferred_element_type=jnp.float32
                )
            return carry

        held[k] = jnp.zeros(held.shape[1:], held.dtype)
        lax.fori_loop(0, slabs, slab, 0)

    def store(k):
        at = pl.ds(pl.multiple_of((k - shared) * size, size), size)
        across = pl.ds(pl.multiple_of(own_place, 128), band_cols)
        return pltpu.make_async_copy(held.at[k], out.at[at, across], out_sem.at[k])

    part_cols = band_cols // PARTS

    def part(ref, p):
        return ref.at[:, pl.ds(p * part_cols, part_cols)]

    def hop(side, k, p):
        return pltpu.make_async_remote_copy(
            src_ref=part(sends.at[side, lax.rem(k, 2)], p),
            dst_ref=part((ups, downs)[side].at[k], p),
            send_sem=(up_send, down_send)[side].at[k, p],
            recv_sem=(up_recv, down_recv)[side].at[k, p],
            device_id={"rep": (here + 1, here - 1)[side]},
            device_id_type=MESH,
        )

    def swap(k):
        return pltpu.make_async_remote_copy(
            src_ref=given.at[k],
            dst_ref=taken.at[k],
            send_sem=pair_send.at[k],
            recv_sem=pair_recv.at[k],
            device_id=twin,
            device_id_type=MESH,
        )

    def store_square():
        across = pl.ds(pl.multiple_of(twin_place, 128), rows)
        return pltpu.make_async_copy(square, out.at[:, across], square_sem)

    def put(source, k, first):
        at = pl.ds(pl.multiple_of(jnp.where(first, 0, half) + k * size, size), size)

        @pl.when(low)
        def _():
            add_strips(square.at[at, :], source)

        @pl.when(jnp.logical_not(low))
        def _():
            def turn(n, carry):
                along = pl.ds(pl.multiple_of(n * 128, 128), 128)
                square[along, at] = source[:, along].astype(jnp.float32).T
                return carry

            lax.fori_loop(0, rows // 128, turn, 0)

    greet([], reps, [twin] if shared else [])
    start(fetch(0, 0, 0))
    multiply(0)

    def tick(t, carry):
        for p in range(PARTS):
            for side, depth in ((0, here), (1, mirror)):
                k = t - depth
                on = (k >= 0) & (k < bands) & (depth < reps - 1)
                pl.when(on & (k >= 2))(lambda: hop(side, k - 2, p).wait_send())
                buffer = part(sends.at[side, lax.rem(k + bands * reps * 2, 2)], p)

                @pl.when(on & (depth == 0))
                def _():
                    add_strips(buffer, part(held.at[k], p))
                    hop(side, k, p).start()

                @pl.when(on & (depth > 0))
                def _():
                    hop(side, k, p).wait_recv()
                    add_strips(buffer, part(held.at[k], p), part((ups, downs)[side].at[k], p))
                    hop(side, k, p).start()

        k = t - jnp.maximum(here, mirror)
        on = (k >= 0) & (k < bands)

        @pl.when(on & (here == 0))
        def _():
            for p in range(PARTS):
                hop(1, k, p).wait_recv()
            add_strips(held.at[k], held.at[k], downs.at[k])

        @pl.when(on & (mirror == 0))
        def _():
            for p in range(PARTS):
                hop(0, k, p).wait_recv()
            add_strips(held.at[k], held.at[k], ups.at[k])

        @pl.when(on & (here > 0) & (mirror > 0))
        def _():
            add_strips(held.at[k], held.at[k], ups.at[k], downs.at[k])

        pl.when(on & (k >= shared))(lambda: store(k).start())
        if shared:

            @pl.when(on & (k < shared))
            def _():
                add_strips(given.at[k], held.at[k])
                swap(k).start()
                put(held.at[k], k, low)

            late = t - jnp.maximum(here, mirror) - LAG

            @pl.when((late >= 0) & (late < shared))
            def _():
                swap(late).wait()
                put(taken.at[late], late, jnp.logical_not(low))
                pl.when(late == shared - 1)(lambda: store_square().start())

        pl.when(t + 1 < bands)(lambda: multiply(t + 1))
        return carry

    lax.fori_loop(0, bands + reps - 1, tick, 0)
    for side, depth in ((0, here), (1, mirror)):
        for k in range(max(bands - 2, 0), bands):
            for p in range(PARTS):
                pl.when(depth < reps - 1)(lambda: hop(side, k, p).wait_send())

    def finish(k, carry):
        store(k).wait()
        return carry

    lax.fori_loop(shared, bands, finish, 0)
    if shared:
        store_square().wait()


def total(summed, rows, cols):
    reps = lax.axis_size("rep")
    paired = cols == 2 * rows and lax.axis_size("row") == 2 * lax.axis_size("col")
    shared = BANDS // 2 if paired else 0
    bands, size = BANDS + shared, rows // BANDS
    band_cols = rows if paired else cols
    depth = summed.shape[0] // SLABS
    dma = pltpu.SemaphoreType.DMA
    shape = (bands, size, band_cols)
    extra = [
        pltpu.VMEM((shared, size, band_cols), jnp.bfloat16),
        pltpu.VMEM((shared, size, band_cols), jnp.bfloat16),
        pltpu.VMEM((rows, rows), jnp.float32),
        dma((max(shared, 1),)),
        dma((max(shared, 1),)),
        dma,
    ]
    return pl.pallas_call(
        functools.partial(total_kernel, reps, rows, cols, shared),
        out_shape=jax.ShapeDtypeStruct((rows, cols), jnp.float32),
        in_specs=[pl.BlockSpec(memory_space=pl.ANY)],
        out_specs=pl.BlockSpec(memory_space=pl.ANY),
        scratch_shapes=[
            pltpu.VMEM(shape, jnp.float32),
            pltpu.VMEM(shape, jnp.bfloat16),
            pltpu.VMEM(shape, jnp.bfloat16),
            pltpu.VMEM((2, 2) + shape[1:], jnp.bfloat16),
            pltpu.VMEM((2, depth, size), summed.dtype),
            pltpu.VMEM((2, depth, band_cols), summed.dtype),
            pltpu.VMEM((size, depth), summed.dtype),
            dma((2,)),
            dma((2,)),
        ]
        + [dma((bands,))]
        + [dma((bands, PARTS))] * 4
        + (extra if paired else []),
        compiler_params=pltpu.CompilerParams(
            collective_id=1, has_side_effects=True, vmem_limit_bytes=VMEM_LIMIT
        ),
    )(summed)


def shards(grad_parts, statistic):
    tile_rows, tile_cols = statistic.shape
    summed = collect(grad_parts[0])
    gram = 0.5 * total(summed, tile_rows, tile_cols)
    return (gram, 0.95 * statistic + 0.05 * gram)


def solution(mesh):
    return jax.shard_map(
        shards,
        mesh=mesh,
        in_specs=(P("rep", ("row", "col"), None), P("row", "col")),
        out_specs=(P("row", "col"), P("row", "col")),
        check_vma=False,
    )
```
